32 devices in a mesh: gx: 8 (over z, y), gy: 4 (over x, core).
Axes of the slice: x: 2, y: 2, z: 4, core: 2. Of those that a mesh axis runs over, the one named last changes fastest.
Arguments:
- populations: float32 [27, 16, 32, 128], P(None, 'gx', 'gy'), as said below
- relax: float32 [27], replicated, may hold values from 0.6 to 1.9
- solid: int32 [16, 32, 128], P('gx', 'gy'), may hold values 0 or 1
- wall_cell: int32 [8, 4, 256], P('gx', 'gy'), may hold values from 0 to 2047, as said below
- wall_normal: int32 [8, 4, 256], P('gx', 'gy'), may hold values from 0 to 5
- wall_count: int32 [8, 4], P('gx', 'gy'), may hold values from 1 to 256, as said below
- sample_ref: int32 [8, 4, 256], P('gx', 'gy'), may hold values from 0 to 255, each once within a row
- stencil_cell: int32 [8, 4, 8, 256], P('gx', 'gy'), may hold values from 0 to 2047, as said below
- stencil_weight: float32 [8, 4, 8, 256], P('gx', 'gy'), may hold values from 0 to 1, as said below
Outputs:
- read: float32 [27, 16, 32, 128], P(None, 'gx', 'gy')
The draws below stay inside these ranges and needn't reach their ends.
Inputs may be any that keep to these rules, and one draw needn't show every extreme that they name: `populations`: positive everywhere. `wall_cell`: the 256 entries of one device are distinct local cells. Slots 0 to wall_count - 1 of a device are live; some device has all 256 live. `stencil_cell`: the eight corners of a unit cube of the owner's local cells, wrapping along z only. `stencil_weight`: nonnegative trilinear weights, summing to one over the eight corners.
All inputs are finite; a program needn't handle non-finite values. No bound on the sum of `solid` on one device may be relied on, other than what follows from the above.
Results may differ from the reference program's by a relative error of at most 0.0003.
Values sent between devices are 32-bit elements; how exact they have to be, the bound alone decides.
A program may use at most 64 MiB of HBM per device.

```python
import math
import jax
import jax.numpy as jnp
import numpy as np
from jax import lax

CX = 2
CY = 8
NZ = 128
SLOTS = 64
WALL = 256
NX = 16
NY = 32
N_GX = 8
N_GY = 4


def draw_populations(key, part):
    base = jax.random.fold_in(key, 101)
    steps = np.array([(a - 1, b - 1, c - 1) for a in range(3) for b in range(3) for c in range(3)]).T
    drift = np.array([0.06, 0.02, -0.02])
    projected = drift @ steps
    resting = 1.0 + 3.0 * projected + 4.5 * projected * projected - 1.5 * np.sum(drift * drift)
    shape = (27, NX, NY, NZ)
    noise = 0.12 * jnp.clip(jax.random.normal(base, shape, jnp.float32), -3.5, 3.5)
    return (jnp.asarray(resting, jnp.float32).reshape(27, 1, 1, 1) * (1.0 + noise)).astype(jnp.float32)


def draw_stencil_cell(key, part):
    grid_x = NX // CX
    grid_y = NY // CY
    shape = (grid_x, grid_y, 1, WALL)
    first, second, third = jax.random.split(jax.random.fold_in(key, 202), 3)
    base_x = jax.random.randint(first, shape, 0, CX - 1)
    base_y = jax.random.randint(second, shape, 0, CY - 1)
    base_z = jax.random.randint(third, shape, 0, NZ)
    corner = jnp.arange(8, dtype=jnp.int32).reshape(1, 1, 8, 1)
    offset_x = corner // 4
    offset_y = corner // 2 % 2
    offset_z = corner % 2
    cells = ((base_x + offset_x) * CY + base_y + offset_y) * NZ + (base_z + offset_z) % NZ
    return cells.astype(jnp.int32)


def draw_stencil_weight(key, part):
    grid_x = NX // CX
    grid_y = NY // CY
    shape = (grid_x, grid_y, 3, 1, WALL)
    base = jax.random.fold_in(key, 303)
    fraction = jax.random.uniform(base, shape, jnp.float32, 0.0, 1.0)
    corner = jnp.arange(8, dtype=jnp.int32)
    bits = jnp.stack([corner // 4, corner // 2 % 2, corner % 2]).reshape(1, 1, 3, 8, 1)
    factor = jnp.where(bits == 1, fraction, 1.0 - fraction)
    return jnp.prod(factor, axis=2).astype(jnp.float32)


def draw_wall_cell(key, part):
    grid_x = NX // CX
    grid_y = NY // CY
    keys = jax.random.split(jax.random.fold_in(key, 404), grid_x * grid_y)
    chosen = jax.vmap(lambda item: jax.random.permutation(item, CX * CY * NZ)[:WALL])(keys)
    return chosen.reshape(grid_x, grid_y, WALL).astype(jnp.int32)


def draw_wall_count(key, part):
    grid_x = NX // CX
    grid_y = NY // CY
    shifted = jax.random.randint(jax.random.fold_in(key, 505), (grid_x, grid_y), 0, 4)
    counts = jnp.right_shift(jnp.full((grid_x, grid_y), WALL, jnp.int32), shifted.astype(jnp.int32))
    counts = jnp.maximum(counts, 1).at[0, 0].set(WALL)
    return counts.astype(jnp.int32)


def plant(result, rng, smallest, top_value):
    dims = result.shape
    spot = [jax.random.randint(jax.random.fold_in(rng, axis), (), 0, dims[axis]) for axis in range(len(dims))]
    result = result.at[tuple(spot)].set(smallest)
    longest = dims.index(max(dims))
    spot[longest] = (spot[longest] + 1) % dims[longest]
    return result.at[tuple(spot)].set(top_value)


def setup_inputs(seed: int = 0) -> dict:
    arg_keys = jax.random.split(jax.random.key(seed), 10)
    populations = draw_populations(jax.random.fold_in(arg_keys[9], 71), 0)
    relax = jnp.clip(jnp.exp(jax.random.uniform(arg_keys[1], (27,), jnp.float32, math.log(0.6), math.log(1.9))), 0.6, 1.9)
    solid = plant((jax.random.randint(arg_keys[2], (NX, NY, NZ), 0, 8) < 1).astype(jnp.int32), jax.random.fold_in(arg_keys[2], 1), 0, 1)
    wall_cell = draw_wall_cell(jax.random.fold_in(arg_keys[9], 71), 0)
    wall_normal = plant(jax.random.randint(arg_keys[4], (N_GX, N_GY, WALL), 0, 6), jax.random.fold_in(arg_keys[4], 1), 0, 5).astype(jnp.int32)
    wall_count = draw_wall_count(jax.random.fold_in(arg_keys[9], 71), 0)
    sample_ref = jax.vmap(lambda own: jax.random.permutation(own, WALL))(jax.random.split(arg_keys[6], N_GX * N_GY)).reshape((N_GX, N_GY, WALL)).astype(jnp.int32)
    stencil_cell = draw_stencil_cell(jax.random.fold_in(arg_keys[9], 71), 0)
    stencil_weight = draw_stencil_weight(jax.random.fold_in(arg_keys[9], 71), 0)
    return {"populations": populations, "relax": relax, "solid": solid, "wall_cell": wall_cell, "wall_normal": wall_normal, "wall_count": wall_count, "sample_ref": sample_ref, "stencil_cell": stencil_cell, "stencil_weight": stencil_weight}


lattice_steps = [(a - 1, b - 1, c - 1) for a in range(3) for b in range(3) for c in range(3)]
wall_ratio = (1.0 / 9.0) ** (1.0 / 7.0)


def lattice():
    steps = np.array(lattice_steps).T
    single = np.where(steps == 0, 2.0 / 3.0, 1.0 / 6.0)
    weights = np.prod(single, axis=0)
    vander = np.array([[1.0, 1.0, 1.0], [-1.0, 0.0, 1.0], [1.0, 0.0, 1.0]])
    undo = np.array([[0.0, -0.5, 0.5], [1.0, 0.0, -1.0], [0.0, 0.5, 0.5]])
    moment = np.kron(np.kron(vander, vander), vander)
    inverse = np.kron(np.kron(undo, undo), undo)
    return (jnp.asarray(steps, jnp.float32), jnp.asarray(weights, jnp.float32),
            jnp.asarray(moment, jnp.float32), jnp.asarray(inverse, jnp.float32))


def moments(pops):
    steps, weights, moment, inverse = lattice()
    scaled = weights[:, None] * pops
    density = jnp.sum(scaled, axis=0)
    momentum = jnp.dot(steps, scaled, precision=lax.Precision.HIGHEST)
    return density, momentum / density[None]


def equilibrium(density, velocity):
    steps, weights, moment, inverse = lattice()
    projected = jnp.dot(steps.T, velocity, precision=lax.Precision.HIGHEST)
    speed_sq = jnp.sum(velocity * velocity, axis=0)
    return density[None] * (1.0 + 3.0 * projected + 4.5 * projected * projected - 1.5 * speed_sq[None])


def collide(pops, relax):
    steps, weights, moment, inverse = lattice()
    scaled = weights[:, None] * pops
    density, velocity = moments(pops)
    balance = weights[:, None] * equilibrium(density, velocity)
    deviation = jnp.dot(moment, scaled - balance, precision=lax.Precision.HIGHEST) * relax[:, None]
    after = scaled - jnp.dot(inverse, deviation, precision=lax.Precision.HIGHEST)
    return after / weights[:, None]


def sample_velocity(velocity, corner_cells, corner_weight):
    picked = velocity[:, corner_cells]
    return jnp.sum(picked * corner_weight[None], axis=1)


def rebuild_columns(columns, density, velocity, normal, live, picked):
    axis_index = normal // 2
    sign = (2 * (normal % 2) - 1).astype(jnp.float32)
    normal_vec = (jnp.arange(3, dtype=jnp.int32)[:, None] == axis_index[None]).astype(jnp.float32) * sign[None]
    along = jnp.sum(picked * normal_vec, axis=0)
    tangential = picked - along[None] * normal_vec
    wall_eq = equilibrium(density, wall_ratio * tangential)
    local_eq = equilibrium(density, velocity)
    return jnp.where(live[None], wall_eq + columns - local_eq, columns)


def rebuild_block(block, density, velocity, cells, normal, live, picked):
    columns = rebuild_columns(block[:, cells], density[cells], velocity[:, cells], normal, live, picked)
    return block.at[:, cells].set(columns)


def to_blocks(field):
    count = field.shape[0]
    field = field.reshape(count, N_GX, CX, N_GY, CY, NZ).transpose(1, 3, 0, 2, 4, 5)
    return field.reshape(N_GX, N_GY, count, CX * CY * NZ)


def from_blocks(blocks):
    count = blocks.shape[2]
    field = blocks.reshape(N_GX, N_GY, count, CX, CY, NZ).transpose(2, 0, 3, 1, 4, 5)
    return field.reshape(count, N_GX * CX, N_GY * CY, NZ)


def reference(populations, relax, solid, wall_cell, wall_normal, wall_count, sample_ref, stencil_cell, stencil_weight):
    blocks = to_blocks(populations)
    density_b, velocity_b = lax.map(lambda row: jax.vmap(moments)(row), blocks)
    samples = jax.vmap(jax.vmap(sample_velocity))(velocity_b, stencil_cell, stencil_weight)
    sent = samples.reshape(N_GX, N_GY, 3, N_GY, SLOTS)
    received = sent.transpose(0, 3, 2, 1, 4).reshape(N_GX, N_GY, 3, N_GY * SLOTS)
    picked = jax.vmap(jax.vmap(lambda table, where_from: table[:, where_from]))(received, sample_ref)
    live = jnp.arange(N_GY * SLOTS, dtype=jnp.int32)[None, None, :] < wall_count[:, :, None]
    rebuilt = jax.vmap(jax.vmap(rebuild_block))(blocks, density_b, velocity_b, wall_cell, wall_normal, live, picked)
    post_b = lax.map(lambda row: jax.vmap(lambda block: collide(block, relax))(row), rebuilt)
    post = from_blocks(post_b)
    outputs = []
    for direction in range(27):
        step_x, step_y, step_z = lattice_steps[direction]
        moved = jnp.roll(post[direction], (step_x, step_y, step_z), axis=(0, 1, 2))
        blocked = jnp.roll(solid, (step_x, step_y, step_z), axis=(0, 1, 2))
        outputs.append(jnp.where(blocked != 0, post[26 - direction], moved))
    return jnp.stack(outputs)
```

```python
import functools

import jax
import jax.numpy as jnp
import numpy as np
from jax import lax
from jax.experimental import pallas as pl
from jax.experimental.pallas import tpu as pltpu
from jax.sharding import PartitionSpec as P

steps = np.array([(a - 1, b - 1, c - 1) for a in range(3) for b in range(3) for c in range(3)])
wall_ratio = (1.0 / 9.0) ** (1.0 / 7.0)
weights = np.prod(np.where(steps == 0, 2.0 / 3.0, 1.0 / 6.0), axis=1)
vander = np.array([[1.0, 1.0, 1.0], [-1.0, 0.0, 1.0], [1.0, 0.0, 1.0]])
moment = np.kron(np.kron(vander, vander), vander)
LANES = 128
MESH = pl.DeviceIdType.MESH


def equilibrium_moments():
    x, y, z = steps.T.astype(float)
    basis = np.stack(
        [
            np.ones(27),
            3 * x,
            3 * y,
            3 * z,
            4.5 * x * x - 1.5,
            4.5 * y * y - 1.5,
            4.5 * z * z - 1.5,
            9 * x * y,
            9 * x * z,
            9 * y * z,
        ],
        axis=1,
    )
    return moment @ (weights[:, None] * basis)


def forward(vals):
    for stride in (9, 3, 1):
        out = list(vals)
        for i in range(27):
            if i // stride % 3 == 0:
                lo, mid, hi = (vals[i], vals[i + stride], vals[i + 2 * stride])
                both = lo + hi
                out[i], out[i + stride], out[i + 2 * stride] = (both + mid, hi - lo, both)
        vals = out
    return vals


def plus(a, b):
    return b if a is None else a if b is None else a + b


def minus(a, b):
    return a if b is None else -b if a is None else a - b


def backward(vals):
    for stride in (9, 3, 1):
        out = list(vals)
        for i in range(27):
            if i // stride % 3 == 0:
                s0, s1, s2 = (vals[i], vals[i + stride], vals[i + 2 * stride])
                out[i], out[i + stride], out[i + 2 * stride] = (
                    minus(s2, s1),
                    minus(s0, s2),
                    plus(s2, s1),
                )
        vals = out
    return vals


def combine(terms):
    total = None
    for factor, value in terms:
        if abs(factor) < 1e-12:
            continue
        if abs(factor - 1.0) < 1e-12:
            total = plus(total, value)
        elif abs(factor + 1.0) < 1e-12:
            total = minus(total, value)
        else:
            total = plus(total, value * np.float32(factor))
    return total


def roll(value, shift, axis):
    return value if shift == 0 else pltpu.roll(value, shift % value.shape[axis], axis)


def lane_gather(row, index):
    return jnp.take_along_axis(
        jnp.broadcast_to(row, index.shape), index, axis=1, mode="promise_in_bounds"
    )


def kernel(
    devices_x,
    devices_y,
    pop_hbm,
    relax,
    solid_hbm,
    wall_hbm,
    normal_hbm,
    count,
    ref_hbm,
    stencil_hbm,
    weight_hbm,
    out,
    pop,
    solid,
    wall,
    normal,
    ref,
    stencil,
    weight,
    vel,
    samples,
    rx,
    post,
    shifted,
    stage_y,
    stage_c,
    stage_s,
    got_x,
    got_y,
    got_c,
    got_sx,
    got_sy,
    got_sc,
    masks,
    load_sem,
    send_sem,
    recv_sem,
):
    size_x, size_y = pop.shape[1:3]
    rows = size_x * size_y
    slots_all = wall.shape[2]
    slots = slots_all // devices_y
    shift_bits = slots.bit_length() - 1
    my_x = lax.axis_index("gx")
    my_y = lax.axis_index("gy")

    def at(dx, dy):
        return {
            "gx": lax.rem(my_x + (dx + devices_x), devices_x),
            "gy": lax.rem(my_y + (dy + devices_y), devices_y),
        }

    loads = [
        pltpu.make_async_copy(src, dst, load_sem.at[n])
        for n, (src, dst) in enumerate(
            [
                (pop_hbm, pop),
                (stencil_hbm, stencil),
                (weight_hbm, weight),
                (solid_hbm, solid),
                (wall_hbm, wall),
                (normal_hbm, normal),
                (ref_hbm, ref),
            ]
        )
    ]
    for load in loads:
        load.start()
    neighbours = [(dx, dy) for dx in (-1, 0, 1) for dy in (-1, 0, 1) if (dx, dy) != (0, 0)]
    greeted = neighbours + [(0, step) for step in range(2, devices_y - 1)]
    barrier = pltpu.get_barrier_semaphore()
    for dx, dy in greeted:
        pl.semaphore_signal(barrier, inc=1, device_id=at(dx, dy), device_id_type=MESH)

    sent = []

    def send(src, dst, dx, dy):
        n = len(sent)
        copy = pltpu.make_async_remote_copy(
            src_ref=src,
            dst_ref=dst,
            send_sem=send_sem.at[n],
            recv_sem=recv_sem.at[n],
            device_id=at(dx, dy),
            device_id_type=MESH,
        )
        copy.start()
        sent.append(copy)
        return copy

    loads[0].wait()
    moments, speeds = ([], [])
    for x in range(size_x):
        found = forward([pop[i, x] * np.float32(weights[i]) for i in range(27)])
        rho = found[0]
        inverse = 1.0 / rho
        u = [found[9] * inverse, found[3] * inverse, found[1] * inverse]
        for c in range(3):
            vel[c * rows + x * size_y : c * rows + (x + 1) * size_y, :] = u[c]
        moments.append(found)
        speeds.append(u)

    loads[1].wait()
    loads[2].wait()
    for tile in range(slots_all // LANES):
        lanes = slice(tile * LANES, (tile + 1) * LANES)
        cell = stencil[0, 0, :, lanes]
        lane = jnp.bitwise_and(cell, LANES - 1)
        row = jnp.right_shift(cell, 7)
        picked = [jnp.zeros(cell.shape, jnp.float32)] * 3
        for r in range(rows):
            here = row == r
            for c in range(3):
                picked[c] = jnp.where(
                    here, lane_gather(vel[c * rows + r : c * rows + r + 1, :], lane), picked[c]
                )
        factor = weight[0, 0, :, lanes]
        for c in range(3):
            samples[tile, c : c + 1, :] = jnp.sum(picked[c] * factor, axis=0, keepdims=True)
    rx[my_y] = samples[(my_y * slots) // LANES]
    pl.semaphore_wait(barrier, len(greeted))
    sample_copies = []
    for step in range(1, devices_y):
        there = lax.rem(my_y + step, devices_y)
        sample_copies.append(send(samples.at[(there * slots) // LANES], rx.at[my_y], 0, step))

    loads[3].wait()
    for side, y in ((0, size_y - 1), (1, 0)):
        for x in range(size_x):
            stage_s[side, x : x + 1, :] = solid[x, y : y + 1, :]
    solid_copies = [
        send(solid.at[size_x - 1], got_sx.at[0], 1, 0),
        send(solid.at[0], got_sx.at[1], -1, 0),
    ]
    for side, dy in ((0, 1), (1, -1)):
        solid_copies.append(send(stage_s.at[side], got_sy.at[side], 0, dy))
        solid_copies.append(send(stage_s.at[side], got_sc.at[0, side], 1, dy))
        solid_copies.append(send(stage_s.at[side], got_sc.at[1, side], -1, dy))

    coefficient = equilibrium_moments()
    for x in range(size_x):
        found, (ux, uy, uz) = (moments[x], speeds[x])
        rho, mx, my, mz = (found[0], found[9], found[3], found[1])
        basis = [rho, mx, my, mz, mx * ux, my * uy, mz * uz, mx * uy, mx * uz, my * uz]
        deviation = []
        for j in range(27):
            if j in (0, 1, 3, 9):
                deviation.append(None)
            else:
                balance = combine(list(zip(coefficient[j], basis)))
                deviation.append(minus(found[j], balance) * relax[j])
        change = backward(deviation)
        for i in range(27):
            half = 0.5 ** int(np.sum(steps[i] != 0)) / weights[i]
            post[i, x] = pop[i, x] - change[i] * np.float32(half)

    for load in loads[4:]:
        load.wait()
    cell = wall[0]
    slot = lax.broadcasted_iota(jnp.int32, (1, slots_all), 1)
    live = slot < count[0, 0]
    which = ref[0]
    offset = lax.rem(my_y * slots, LANES)
    row_hit = jnp.logical_and(
        lax.broadcasted_iota(jnp.int32, (rows, slots_all), 0) == jnp.right_shift(cell, 7), live
    )
    values = [
        jnp.right_shift(which, shift_bits) + 1,
        jnp.bitwise_and(which, slots - 1) + offset,
        jnp.right_shift(normal[0], 1),
    ]
    left = jnp.concatenate(
        [jnp.where(row_hit, value.astype(jnp.float32), 0.0) for value in values], axis=0
    ).astype(jnp.bfloat16)
    right = jnp.where(
        lax.broadcasted_iota(jnp.int32, (LANES, slots_all), 0)
        == jnp.bitwise_and(cell, LANES - 1),
        1.0,
        0.0,
    ).astype(jnp.bfloat16)
    table = lax.dot_general(
        left, right, (((1,), (1,)), ((), ())), preferred_element_type=jnp.float32
    ).astype(jnp.int32)

    for copy in sample_copies:
        copy.wait_recv()
    for x in range(size_x):
        part = [table[n * rows + x * size_y : n * rows + (x + 1) * size_y] for n in range(3)]
        source, lane, axis = part
        rho, u = (moments[x][0], speeds[x])
        new = []
        for c in range(3):
            value = jnp.zeros((size_y, LANES), jnp.float32)
            for peer in range(devices_y):
                value = jnp.where(
                    source == peer + 1, lane_gather(rx[peer, c : c + 1, :], lane), value
                )
            value = jnp.where(axis == c, 0.0, value * np.float32(wall_ratio))
            new.append(jnp.where(source > 0, value, u[c]))
        linear = [3.0 * rho * (new[c] - u[c]) for c in range(3)]
        pure = [rho * (new[c] * new[c] - u[c] * u[c]) for c in range(3)]
        rest = -1.5 * (pure[0] + pure[1] + pure[2])
        pure = [4.5 * value for value in pure]
        mixed = {
            (c, d): 9.0 * rho * (new[c] * new[d] - u[c] * u[d])
            for c, d in ((0, 1), (0, 2), (1, 2))
        }
        for i in range(14):
            step = steps[i]
            used = [c for c in range(3) if step[c] != 0]
            even, odd = (rest, None)
            for c in used:
                even = even + pure[c]
                odd = plus(odd, linear[c]) if step[c] > 0 else minus(odd, linear[c])
            for c, d in mixed:
                if step[c] * step[d] > 0:
                    even = even + mixed[c, d]
                elif step[c] * step[d] < 0:
                    even = even - mixed[c, d]
            if odd is None:
                post[i, x] = post[i, x] + even
            else:
                post[i, x] = post[i, x] + (even + odd)
                post[26 - i, x] = post[26 - i, x] + (even - odd)
        for i in range(27):
            a, b, c = steps[i]
            value = roll(roll(post[i, x], b, 0), c, 1)
            shifted[i, x] = value
            if b != 0:
                side = 0 if b > 0 else 1
                edge = 0 if b > 0 else size_y - 1
                line = value[edge : edge + 1, :]
                if 0 <= x + a < size_x:
                    n = ((a + 1) * 3 + c + 1) * size_x + x
                    stage_y[side, n : n + 1, :] = line
                else:
                    stage_c[0 if a > 0 else 1, side, c + 1 : c + 2, :] = line

    halo = [
        send(shifted.at[18:27, size_x - 1], got_x.at[0], 1, 0),
        send(shifted.at[0:9, 0], got_x.at[1], -1, 0),
    ]
    for side, dy in ((0, 1), (1, -1)):
        for way, dx in ((0, 1), (1, -1)):
            halo.append(send(stage_c.at[way, side], got_c.at[way, side], dx, dy))
    for side, dy in ((0, 1), (1, -1)):
        halo.append(send(stage_y.at[side], got_y.at[side], 0, dy))

    for copy in solid_copies:
        copy.wait_recv()
    line_of = lax.broadcasted_iota(jnp.int32, (size_y, LANES), 0)

    def mend(value, line, b):
        edge = 0 if b > 0 else size_y - 1
        return jnp.where(line_of == edge, jnp.broadcast_to(line, value.shape), value)

    for x in range(-1, size_x + 1):
        plane = got_sx[0] if x < 0 else got_sx[1] if x == size_x else solid[x]
        for b in (-1, 0, 1):
            value = roll(plane, b, 0)
            if b != 0:
                side = 0 if b > 0 else 1
                if x < 0:
                    line = got_sc[0, side, size_x - 1 : size_x, :]
                elif x == size_x:
                    line = got_sc[1, side, 0:1, :]
                else:
                    line = got_sy[side, x : x + 1, :]
                value = mend(value, line, b)
            for c in (-1, 0, 1):
                masks[(b + 1) * 3 + c + 1, x + 1] = roll(value, c, 1)

    for copy in halo:
        copy.wait_recv()
    for i in range(27):
        a, b, c = steps[i]
        way = 0 if a > 0 else 1
        side = 0 if b > 0 else 1
        for x in range(size_x):
            origin = x - a
            if 0 <= origin < size_x:
                value = shifted[i, origin]
                n = ((a + 1) * 3 + c + 1) * size_x + origin
                line = got_y[side, n : n + 1, :] if b != 0 else None
            else:
                value = got_x[way, i % 9]
                line = got_c[way, side, c + 1 : c + 2, :] if b != 0 else None
            if b != 0:
                value = mend(value, line, b)
            blocked = masks[(b + 1) * 3 + c + 1, origin + 1] != 0
            out[i, x] = jnp.where(blocked, post[26 - i, x], value)
    for copy in sent:
        copy.wait_send()


def local(populations, relax, solid, wall_cell, wall_normal, wall_count, sample_ref, cells, factors):
    devices_x, devices_y = (lax.axis_size("gx"), lax.axis_size("gy"))
    size_x, size_y, size_z = populations.shape[1:]
    slots_all = wall_cell.shape[2]
    slots = slots_all // devices_y
    assert size_z == LANES and LANES % slots == 0 and slots & (slots - 1) == 0
    assert slots_all % LANES == 0 and devices_x > 2 and devices_y > 2
    f32, i32 = (jnp.float32, jnp.int32)
    lines = -(-9 * size_x // 8) * 8
    sends = devices_y - 1 + 16
    vmem = pltpu.VMEM
    tile = (size_y, LANES)
    anywhere = pl.BlockSpec(memory_space=pl.ANY)
    smem = pl.BlockSpec(memory_space=pltpu.SMEM)
    return pl.pallas_call(
        functools.partial(kernel, devices_x, devices_y),
        out_shape=jax.ShapeDtypeStruct(populations.shape, f32),
        in_specs=[
            anywhere,
            smem,
            anywhere,
            anywhere,
            anywhere,
            smem,
            anywhere,
            anywhere,
            anywhere,
        ],
        out_specs=pl.BlockSpec(memory_space=pltpu.VMEM),
        scratch_shapes=[
            vmem(populations.shape, f32),
            vmem(solid.shape, i32),
            vmem(wall_cell.shape, i32),
            vmem(wall_normal.shape, i32),
            vmem(sample_ref.shape, i32),
            vmem(cells.shape, i32),
            vmem(factors.shape, f32),
            vmem((3 * size_x * size_y, LANES), f32),
            vmem((slots_all // LANES, 8, LANES), f32),
            vmem((devices_y, 8, LANES), f32),
            vmem(populations.shape, f32),
            vmem(populations.shape, f32),
            vmem((2, lines, LANES), f32),
            vmem((2, 2, 8, LANES), f32),
            vmem((2, 8, LANES), i32),
            vmem((2, 9) + tile, f32),
            vmem((2, lines, LANES), f32),
            vmem((2, 2, 8, LANES), f32),
            vmem((2,) + tile, i32),
            vmem((2, 8, LANES), i32),
            vmem((2, 2, 8, LANES), i32),
            vmem((9, size_x + 2) + tile, i32),
            pltpu.SemaphoreType.DMA((7,)),
            pltpu.SemaphoreType.DMA((sends,)),
            pltpu.SemaphoreType.DMA((sends,)),
        ],
        compiler_params=pltpu.CompilerParams(collective_id=0, has_side_effects=True),
        name="lattice_step",
    )(populations, relax, solid, wall_cell, wall_normal, wall_count, sample_ref, cells, factors)


def solution(mesh):
    return jax.shard_map(
        local,
        mesh=mesh,
        in_specs=(
            P(None, "gx", "gy", None),
            P(),
            P("gx", "gy", None),
            P("gx", "gy", None),
            P("gx", "gy", None),
            P("gx", "gy"),
            P("gx", "gy", None),
            P("gx", "gy", None, None),
            P("gx", "gy", None, None),
        ),
        out_specs=P(None, "gx", "gy", None),
        check_vma=False,
    )
```

```python
import functools

import jax
import jax.numpy as jnp
import numpy as np
from jax import lax
from jax.experimental import pallas as pl
from jax.experimental.pallas import tpu as pltpu
from jax.sharding import PartitionSpec as P

steps = np.array([(a - 1, b - 1, c - 1) for a in range(3) for b in range(3) for c in range(3)])
wall_ratio = (1.0 / 9.0) ** (1.0 / 7.0)
weights = np.prod(np.where(steps == 0, 2.0 / 3.0, 1.0 / 6.0), axis=1)
vander = np.array([[1.0, 1.0, 1.0], [-1.0, 0.0, 1.0], [1.0, 0.0, 1.0]])
moment = np.kron(np.kron(vander, vander), vander)
LANES = 128
MESH = pl.DeviceIdType.MESH


def equilibrium_moments():
    x, y, z = steps.T.astype(float)
    basis = np.stack(
        [
            np.ones(27),
            3 * x,
            3 * y,
            3 * z,
            4.5 * x * x - 1.5,
            4.5 * y * y - 1.5,
            4.5 * z * z - 1.5,
            9 * x * y,
            9 * x * z,
            9 * y * z,
        ],
        axis=1,
    )
    return moment @ (weights[:, None] * basis)


def forward(vals):
    for stride in (9, 3, 1):
        out = list(vals)
        for i in range(27):
            if i // stride % 3 == 0:
                lo, mid, hi = (vals[i], vals[i + stride], vals[i + 2 * stride])
                both = lo + hi
                out[i], out[i + stride], out[i + 2 * stride] = (both + mid, hi - lo, both)
        vals = out
    return vals


def plus(a, b):
    return b if a is None else a if b is None else a + b


def minus(a, b):
    return a if b is None else -b if a is None else a - b


def backward(vals):
    for stride in (9, 3, 1):
        out = list(vals)
        for i in range(27):
            if i // stride % 3 == 0:
                s0, s1, s2 = (vals[i], vals[i + stride], vals[i + 2 * stride])
                out[i], out[i + stride], out[i + 2 * stride] = (
                    minus(s2, s1),
                    minus(s0, s2),
                    plus(s2, s1),
                )
        vals = out
    return vals


def combine(terms):
    total = None
    for factor, value in terms:
        if abs(factor) < 1e-12:
            continue
        if abs(factor - 1.0) < 1e-12:
            total = plus(total, value)
        elif abs(factor + 1.0) < 1e-12:
            total = minus(total, value)
        else:
            total = plus(total, value * np.float32(factor))
    return total


def roll(value, shift, axis):
    return value if shift == 0 else pltpu.roll(value, shift % value.shape[axis], axis)


def lane_gather(row, index):
    return jnp.take_along_axis(
        jnp.broadcast_to(row, index.shape), index, axis=1, mode="promise_in_bounds"
    )


def kernel(
    devices_x,
    devices_y,
    pop_hbm,
    relax,
    solid_hbm,
    wall_hbm,
    normal_hbm,
    count,
    ref_hbm,
    stencil_hbm,
    weight_hbm,
    out,
    pop,
    solid,
    wall,
    normal,
    ref,
    stencil,
    weight,
    vel,
    samples,
    rx,
    post,
    settled,
    fields,
    fresh,
    shifted,
    stage_y,
    stage_c,
    stage_s,
    stage_f,
    stage_n,
    got_x,
    got_y,
    got_c,
    got_sx,
    got_sy,
    got_sc,
    got_fx,
    got_fy,
    got_fc,
    got_nx,
    got_ny,
    got_nc,
    lines,
    line_fields,
    line_fresh,
    masks,
    load_sem,
    send_sem,
    recv_sem,
):
    size_x, size_y = pop.shape[1:3]
    rows = size_x * size_y
    slots_all = wall.shape[2]
    slots = slots_all // devices_y
    shift_bits = slots.bit_length() - 1
    my_x = lax.axis_index("gx")
    my_y = lax.axis_index("gy")

    def at(dx, dy):
        return {
            "gx": lax.rem(my_x + (dx + devices_x), devices_x),
            "gy": lax.rem(my_y + (dy + devices_y), devices_y),
        }

    loads = [
        pltpu.make_async_copy(src, dst, load_sem.at[n])
        for n, (src, dst) in enumerate(
            [
                (pop_hbm, pop),
                (stencil_hbm, stencil),
                (weight_hbm, weight),
                (solid_hbm, solid),
                (wall_hbm, wall),
                (normal_hbm, normal),
                (ref_hbm, ref),
            ]
        )
    ]
    for load in loads:
        load.start()
    neighbours = [(dx, dy) for dx in (-1, 0, 1) for dy in (-1, 0, 1) if (dx, dy) != (0, 0)]
    greeted = neighbours + [(0, step) for step in range(2, devices_y - 1)]
    barrier = pltpu.get_barrier_semaphore()
    for dx, dy in greeted:
        pl.semaphore_signal(barrier, inc=1, device_id=at(dx, dy), device_id_type=MESH)

    sent = []

    def send(src, dst, dx, dy):
        n = len(sent)
        copy = pltpu.make_async_remote_copy(
            src_ref=src,
            dst_ref=dst,
            send_sem=send_sem.at[n],
            recv_sem=recv_sem.at[n],
            device_id=at(dx, dy),
            device_id_type=MESH,
        )
        copy.start()
        sent.append(copy)
        return copy

    loads[0].wait()
    moments, speeds = ([], [])
    for x in range(size_x):
        found = forward([pop[i, x] * np.float32(weights[i]) for i in range(27)])
        rho = found[0]
        inverse = 1.0 / rho
        u = [found[9] * inverse, found[3] * inverse, found[1] * inverse]
        for c in range(3):
            vel[c * rows + x * size_y : c * rows + (x + 1) * size_y, :] = u[c]
        for f, value in enumerate([rho] + u):
            fields[f, x] = value
        moments.append(found)
        speeds.append(u)

    loads[1].wait()
    loads[2].wait()
    for tile in range(slots_all // LANES):
        lanes = slice(tile * LANES, (tile + 1) * LANES)
        cell = stencil[0, 0, :, lanes]
        lane = jnp.bitwise_and(cell, LANES - 1)
        row = jnp.right_shift(cell, 7)
        picked = [jnp.zeros(cell.shape, jnp.float32)] * 3
        for r in range(rows):
            here = row == r
            for c in range(3):
                picked[c] = jnp.where(
                    here, lane_gather(vel[c * rows + r : c * rows + r + 1, :], lane), picked[c]
                )
        factor = weight[0, 0, :, lanes]
        for c in range(3):
            samples[tile, c : c + 1, :] = jnp.sum(picked[c] * factor, axis=0, keepdims=True)
    rx[my_y] = samples[(my_y * slots) // LANES]
    pl.semaphore_wait(barrier, len(greeted))
    sample_copies = []
    for step in range(1, devices_y):
        there = lax.rem(my_y + step, devices_y)
        sample_copies.append(send(samples.at[(there * slots) // LANES], rx.at[my_y], 0, step))

    loads[3].wait()
    for side, y in ((0, size_y - 1), (1, 0)):
        for x in range(size_x):
            stage_s[side, x : x + 1, :] = solid[x, y : y + 1, :]
    solid_copies = [
        send(solid.at[size_x - 1], got_sx.at[0], 1, 0),
        send(solid.at[0], got_sx.at[1], -1, 0),
    ]
    for side, dy in ((0, 1), (1, -1)):
        solid_copies.append(send(stage_s.at[side], got_sy.at[side], 0, dy))
        solid_copies.append(send(stage_s.at[side], got_sc.at[0, side], 1, dy))
        solid_copies.append(send(stage_s.at[side], got_sc.at[1, side], -1, dy))

    coefficient = equilibrium_moments()
    for x in range(size_x):
        found, (ux, uy, uz) = (moments[x], speeds[x])
        rho, mx, my, mz = (found[0], found[9], found[3], found[1])
        basis = [rho, mx, my, mz, mx * ux, my * uy, mz * uz, mx * uy, mx * uz, my * uz]
        deviation = []
        for j in range(27):
            if j in (0, 1, 3, 9):
                deviation.append(None)
            else:
                balance = combine(list(zip(coefficient[j], basis)))
                deviation.append(minus(found[j], balance) * relax[j])
        change = backward(deviation)
        for i in range(27):
            half = 0.5 ** int(np.sum(steps[i] != 0)) / weights[i]
            post[i, x] = pop[i, x] - change[i] * np.float32(half)

    for i in range(27):
        a, b, c = steps[i]
        if b == 0:
            continue
        side = 0 if b > 0 else 1
        edge = size_y - 1 if b > 0 else 0
        for x in range(size_x):
            line = post[i, x, edge : edge + 1, :]
            if 0 <= x + a < size_x:
                n = ((a + 1) * 3 + c + 1) * size_x + x
                stage_y[side, n : n + 1, :] = line
            else:
                stage_c[0 if a > 0 else 1, side, c + 1 : c + 2, :] = line
    for side, y in ((0, size_y - 1), (1, 0)):
        for f in range(4):
            for x in range(size_x):
                n = f * size_x + x
                stage_f[side, n : n + 1, :] = fields[f, x, y : y + 1, :]
    early = [
        send(post.at[18:27, size_x - 1], got_x.at[0], 1, 0),
        send(post.at[0:9, 0], got_x.at[1], -1, 0),
        send(fields.at[:, size_x - 1], got_fx.at[0], 1, 0),
        send(fields.at[:, 0], got_fx.at[1], -1, 0),
    ]
    for side, dy in ((0, 1), (1, -1)):
        for way, dx in ((0, 1), (1, -1)):
            early.append(send(stage_c.at[way, side], got_c.at[way, side], dx, dy))
            early.append(send(stage_f.at[side], got_fc.at[way, side], dx, dy))
        early.append(send(stage_y.at[side], got_y.at[side], 0, dy))
        early.append(send(stage_f.at[side], got_fy.at[side], 0, dy))

    for load in loads[4:]:
        load.wait()
    cell = wall[0]
    slot = lax.broadcasted_iota(jnp.int32, (1, slots_all), 1)
    live = slot < count[0, 0]
    which = ref[0]
    offset = lax.rem(my_y * slots, LANES)
    row_hit = jnp.logical_and(
        lax.broadcasted_iota(jnp.int32, (rows, slots_all), 0) == jnp.right_shift(cell, 7), live
    )
    values = [
        jnp.right_shift(which, shift_bits) + 1,
        jnp.bitwise_and(which, slots - 1) + offset,
        jnp.right_shift(normal[0], 1),
    ]
    left = jnp.concatenate(
        [jnp.where(row_hit, value.astype(jnp.float32), 0.0) for value in values], axis=0
    ).astype(jnp.bfloat16)
    right = jnp.where(
        lax.broadcasted_iota(jnp.int32, (LANES, slots_all), 0)
        == jnp.bitwise_and(cell, LANES - 1),
        1.0,
        0.0,
    ).astype(jnp.bfloat16)
    table = lax.dot_general(
        left, right, (((1,), (1,)), ((), ())), preferred_element_type=jnp.float32
    ).astype(jnp.int32)

    for copy in sample_copies:
        copy.wait_recv()
    for x in range(size_x):
        part = [table[n * rows + x * size_y : n * rows + (x + 1) * size_y] for n in range(3)]
        source, lane, axis = part
        for c in range(3):
            value = jnp.zeros((size_y, LANES), jnp.float32)
            for peer in range(devices_y):
                value = jnp.where(
                    source == peer + 1, lane_gather(rx[peer, c : c + 1, :], lane), value
                )
            value = jnp.where(axis == c, 0.0, value * np.float32(wall_ratio))
            value = jnp.where(source > 0, value, speeds[x][c])
            fresh[c, x] = value
            for side, y in ((0, size_y - 1), (1, 0)):
                n = c * size_x + x
                stage_n[side, n : n + 1, :] = value[y : y + 1, :]
    late = [
        send(fresh.at[:, size_x - 1], got_nx.at[0], 1, 0),
        send(fresh.at[:, 0], got_nx.at[1], -1, 0),
    ]
    for side, dy in ((0, 1), (1, -1)):
        late.append(send(stage_n.at[side], got_nc.at[0, side], 1, dy))
        late.append(send(stage_n.at[side], got_nc.at[1, side], -1, dy))
    for side, dy in ((0, 1), (1, -1)):
        late.append(send(stage_n.at[side], got_ny.at[side], 0, dy))

    def correction(rho, u, new, wanted):
        linear = [3.0 * rho * (new[c] - u[c]) for c in range(3)]
        pure = [rho * (new[c] * new[c] - u[c] * u[c]) for c in range(3)]
        rest = -1.5 * (pure[0] + pure[1] + pure[2])
        pure = [4.5 * value for value in pure]
        mixed = {
            (c, d): 9.0 * rho * (new[c] * new[d] - u[c] * u[d])
            for c, d in ((0, 1), (0, 2), (1, 2))
        }
        halves, found = ({}, {})
        for i in wanted:
            first = min(i, 26 - i)
            if first not in halves:
                step = steps[first]
                even, odd = (rest, None)
                for c in range(3):
                    if step[c] != 0:
                        even = even + pure[c]
                        odd = plus(odd, linear[c]) if step[c] > 0 else minus(odd, linear[c])
                for c, d in mixed:
                    if step[c] * step[d] > 0:
                        even = even + mixed[c, d]
                    elif step[c] * step[d] < 0:
                        even = even - mixed[c, d]
                halves[first] = (even, odd)
            even, odd = halves[first]
            found[i] = even if odd is None else even + odd if i == first else even - odd
        return found

    for x in range(size_x):
        found = correction(
            fields[0, x], [fields[1 + c, x] for c in range(3)], [fresh[c, x] for c in range(3)], range(27)
        )
        for i in range(27):
            a, b, c = steps[i]
            value = post[i, x] + found[i]
            settled[i, x] = value
            shifted[i, x] = roll(roll(value, b, 0), c, 1)

    for copy in solid_copies:
        copy.wait_recv()
    line_of = lax.broadcasted_iota(jnp.int32, (size_y, LANES), 0)

    def mend(value, line, b):
        edge = 0 if b > 0 else size_y - 1
        return jnp.where(line_of == edge, jnp.broadcast_to(line, value.shape), value)

    for x in range(-1, size_x + 1):
        plane = got_sx[0] if x < 0 else got_sx[1] if x == size_x else solid[x]
        for b in (-1, 0, 1):
            value = roll(plane, b, 0)
            if b != 0:
                side = 0 if b > 0 else 1
                if x < 0:
                    line = got_sc[0, side, size_x - 1 : size_x, :]
                elif x == size_x:
                    line = got_sc[1, side, 0:1, :]
                else:
                    line = got_sy[side, x : x + 1, :]
                value = mend(value, line, b)
            for c in (-1, 0, 1):
                masks[(b + 1) * 3 + c + 1, x + 1] = roll(value, c, 1)

    def gather_rows(target, index, straight, corner, f):
        for x in range(size_x):
            n = f * size_x + x
            target[index + (slice(x, x + 1),)] = straight[n : n + 1, :]
        n = f * size_x + size_x - 1
        target[index + (slice(size_x, size_x + 1),)] = corner[0][n : n + 1, :]
        n = f * size_x
        target[index + (slice(size_x + 1, size_x + 2),)] = corner[1][n : n + 1, :]

    for copy in early:
        copy.wait_recv()
    for side in range(2):
        for j in range(9):
            a, c = (j // 3 - 1, j % 3 - 1)
            for x in range(size_x):
                if 0 <= x + a < size_x:
                    n = j * size_x + x
                    lines[side, j, x : x + 1, :] = got_y[side, n : n + 1, :]
            if a != 0:
                way = 0 if a > 0 else 1
                lines[side, j, size_x + way : size_x + way + 1, :] = got_c[
                    way, side, c + 1 : c + 2, :
                ]
        for f in range(4):
            gather_rows(
                line_fields, (side, f), got_fy.at[side], [got_fc.at[way, side] for way in (0, 1)], f
            )

    for copy in late:
        copy.wait_recv()
    border = {}
    for side, b in ((0, 1), (1, -1)):
        for c in range(3):
            gather_rows(
                line_fresh, (side, c), got_ny.at[side], [got_nc.at[way, side] for way in (0, 1)], c
            )
        wanted = [i for i in range(27) if steps[i][1] == b]
        found = correction(
            line_fields[side, 0],
            [line_fields[side, 1 + c] for c in range(3)],
            [line_fresh[side, c] for c in range(3)],
            wanted,
        )
        for i in wanted:
            a, _, c = steps[i]
            border[i] = roll(lines[side, (a + 1) * 3 + c + 1] + found[i], c, 1)
    planes = {}
    for way, a in ((0, 1), (1, -1)):
        wanted = [i for i in range(27) if steps[i][0] == a]
        found = correction(
            got_fx[way, 0],
            [got_fx[way, 1 + c] for c in range(3)],
            [got_nx[way, c] for c in range(3)],
            wanted,
        )
        for i in wanted:
            _, b, c = steps[i]
            planes[i] = roll(roll(got_x[way, i % 9] + found[i], b, 0), c, 1)
    for i in range(27):
        a, b, c = steps[i]
        for x in range(size_x):
            origin = x - a
            inside = 0 <= origin < size_x
            value = shifted[i, origin] if inside else planes[i]
            if b != 0:
                n = origin if inside else size_x + (0 if a > 0 else 1)
                value = mend(value, border[i][n : n + 1, :], b)
            blocked = masks[(b + 1) * 3 + c + 1, origin + 1] != 0
            out[i, x] = jnp.where(blocked, settled[26 - i, x], value)
    for copy in sent:
        copy.wait_send()


def write_out(source, out, sem):
    copy = pltpu.make_async_copy(source, out, sem)
    copy.start()
    copy.wait()


def local(populations, relax, solid, wall_cell, wall_normal, wall_count, sample_ref, cells, factors):
    devices_x, devices_y = (lax.axis_size("gx"), lax.axis_size("gy"))
    size_x, size_y, size_z = populations.shape[1:]
    slots_all = wall_cell.shape[2]
    slots = slots_all // devices_y
    assert size_z == LANES and LANES % slots == 0 and slots & (slots - 1) == 0
    assert slots_all % LANES == 0 and devices_x > 2 and devices_y > 2
    f32, i32 = (jnp.float32, jnp.int32)
    lines = -(-9 * size_x // 8) * 8
    assert size_x + 2 <= 8
    few = -(-4 * size_x // 8) * 8
    sends = devices_y - 1 + 8 + 16 + 8
    vmem = pltpu.VMEM
    tile = (size_y, LANES)
    anywhere = pl.BlockSpec(memory_space=pl.ANY)
    smem = pl.BlockSpec(memory_space=pltpu.SMEM)
    result = pl.pallas_call(
        functools.partial(kernel, devices_x, devices_y),
        out_shape=pltpu.VMEM(populations.shape, f32),
        in_specs=[
            anywhere,
            smem,
            anywhere,
            anywhere,
            anywhere,
            smem,
            anywhere,
            anywhere,
            anywhere,
        ],
        out_specs=pl.BlockSpec(memory_space=pltpu.VMEM),
        scratch_shapes=[
            vmem(populations.shape, f32),
            vmem(solid.shape, i32),
            vmem(wall_cell.shape, i32),
            vmem(wall_normal.shape, i32),
            vmem(sample_ref.shape, i32),
            vmem(cells.shape, i32),
            vmem(factors.shape, f32),
            vmem((3 * size_x * size_y, LANES), f32),
            vmem((slots_all // LANES, 8, LANES), f32),
            vmem((devices_y, 8, LANES), f32),
            vmem(populations.shape, f32),
            vmem(populations.shape, f32),
            vmem((4, size_x) + tile, f32),
            vmem((3, size_x) + tile, f32),
            vmem(populations.shape, f32),
            vmem((2, lines, LANES), f32),
            vmem((2, 2, 8, LANES), f32),
            vmem((2, 8, LANES), i32),
            vmem((2, few, LANES), f32),
            vmem((2, few, LANES), f32),
            vmem((2, 9) + tile, f32),
            vmem((2, lines, LANES), f32),
            vmem((2, 2, 8, LANES), f32),
            vmem((2,) + tile, i32),
            vmem((2, 8, LANES), i32),
            vmem((2, 2, 8, LANES), i32),
            vmem((2, 4) + tile, f32),
            vmem((2, few, LANES), f32),
            vmem((2, 2, few, LANES), f32),
            vmem((2, 3) + tile, f32),
            vmem((2, few, LANES), f32),
            vmem((2, 2, few, LANES), f32),
            vmem((2, 9, 8, LANES), f32),
            vmem((2, 4, 8, LANES), f32),
            vmem((2, 3, 8, LANES), f32),
            vmem((9, size_x + 2) + tile, i32),
            pltpu.SemaphoreType.DMA((7,)),
            pltpu.SemaphoreType.DMA((sends,)),
            pltpu.SemaphoreType.DMA((sends,)),
        ],
        compiler_params=pltpu.CompilerParams(collective_id=0, has_side_effects=True),
        name="lattice_step",
    )(populations, relax, solid, wall_cell, wall_normal, wall_count, sample_ref, cells, factors)
    result = pltpu.with_memory_space_constraint(result, pltpu.VMEM)
    return pl.pallas_call(
        write_out,
        out_shape=jax.ShapeDtypeStruct(populations.shape, f32),
        in_specs=[pl.BlockSpec(memory_space=pltpu.VMEM)],
        out_specs=anywhere,
        scratch_shapes=[pltpu.SemaphoreType.DMA],
        name="write_out",
    )(result)


def solution(mesh):
    return jax.shard_map(
        local,
        mesh=mesh,
        in_specs=(
            P(None, "gx", "gy", None),
            P(),
            P("gx", "gy", None),
            P("gx", "gy", None),
            P("gx", "gy", None),
            P("gx", "gy"),
            P("gx", "gy", None),
            P("gx", "gy", None, None),
            P("gx", "gy", None, None),
        ),
        out_specs=P(None, "gx", "gy", None),
        check_vma=False,
    )
```

```python
import functools

import jax
import jax.numpy as jnp
import numpy as np
from jax import lax
from jax.experimental import pallas as pl
from jax.experimental.pallas import tpu as pltpu
from jax.sharding import PartitionSpec as P

steps = np.array([(a - 1, b - 1, c - 1) for a in range(3) for b in range(3) for c in range(3)])
wall_ratio = (1.0 / 9.0) ** (1.0 / 7.0)
weights = np.prod(np.where(steps == 0, 2.0 / 3.0, 1.0 / 6.0), axis=1)
vander = np.array([[1.0, 1.0, 1.0], [-1.0, 0.0, 1.0], [1.0, 0.0, 1.0]])
moment = np.kron(np.kron(vander, vander), vander)
LANES = 128
MESH = pl.DeviceIdType.MESH


def equilibrium_moments():
    x, y, z = steps.T.astype(float)
    basis = np.stack(
        [
            np.ones(27),
            3 * x,
            3 * y,
            3 * z,
            4.5 * x * x - 1.5,
            4.5 * y * y - 1.5,
            4.5 * z * z - 1.5,
            9 * x * y,
            9 * x * z,
            9 * y * z,
        ],
        axis=1,
    )
    return moment @ (weights[:, None] * basis)


def forward(vals):
    for stride in (9, 3, 1):
        out = list(vals)
        for i in range(27):
            if i // stride % 3 == 0:
                lo, mid, hi = (vals[i], vals[i + stride], vals[i + 2 * stride])
                both = lo + hi
                out[i], out[i + stride], out[i + 2 * stride] = (both + mid, hi - lo, both)
        vals = out
    return vals


def plus(a, b):
    return b if a is None else a if b is None else a + b


def minus(a, b):
    return a if b is None else -b if a is None else a - b


def backward(vals):
    for stride in (9, 3, 1):
        out = list(vals)
        for i in range(27):
            if i // stride % 3 == 0:
                s0, s1, s2 = (vals[i], vals[i + stride], vals[i + 2 * stride])
                out[i], out[i + stride], out[i + 2 * stride] = (
                    minus(s2, s1),
                    minus(s0, s2),
                    plus(s2, s1),
                )
        vals = out
    return vals


def combine(terms):
    total = None
    for factor, value in terms:
        if abs(factor) < 1e-12:
            continue
        if abs(factor - 1.0) < 1e-12:
            total = plus(total, value)
        elif abs(factor + 1.0) < 1e-12:
            total = minus(total, value)
        else:
            total = plus(total, value * np.float32(factor))
    return total


def roll(value, shift, axis):
    return value if shift == 0 else pltpu.roll(value, shift % value.shape[axis], axis)


def lane_gather(row, index):
    return jnp.take_along_axis(
        jnp.broadcast_to(row, index.shape), index, axis=1, mode="promise_in_bounds"
    )


def kernel(
    devices_x,
    devices_y,
    pop_hbm,
    relax,
    solid_hbm,
    wall_hbm,
    normal_hbm,
    count,
    ref_hbm,
    stencil_hbm,
    weight_hbm,
    out,
    pop,
    solid,
    wall,
    normal,
    ref,
    stencil,
    weight,
    vel,
    samples,
    rx,
    post,
    settled,
    fields,
    shifted,
    stage_y,
    stage_c,
    stage_s,
    stage_f,
    got_x,
    got_y,
    got_c,
    got_sx,
    got_sy,
    got_sc,
    got_fx,
    got_fy,
    got_fc,
    lines,
    line_fields,
    masks,
    load_sem,
    send_sem,
    recv_sem,
):
    size_x, size_y = pop.shape[1:3]
    rows = size_x * size_y
    slots_all = wall.shape[2]
    slots = slots_all // devices_y
    shift_bits = slots.bit_length() - 1
    my_x = lax.axis_index("gx")
    my_y = lax.axis_index("gy")

    def at(dx, dy):
        return {
            "gx": lax.rem(my_x + (dx + devices_x), devices_x),
            "gy": lax.rem(my_y + (dy + devices_y), devices_y),
        }

    loads = [
        pltpu.make_async_copy(src, dst, load_sem.at[n])
        for n, (src, dst) in enumerate(
            [
                (pop_hbm, pop),
                (stencil_hbm, stencil),
                (weight_hbm, weight),
                (solid_hbm, solid),
                (wall_hbm, wall),
                (normal_hbm, normal),
                (ref_hbm, ref),
            ]
        )
    ]
    for load in loads:
        load.start()
    greeted = [(dx, dy) for dx in (-1, 0, 1) for dy in range(devices_y) if (dx, dy) != (0, 0)]
    barrier = pltpu.get_barrier_semaphore()
    for dx, dy in greeted:
        pl.semaphore_signal(barrier, inc=1, device_id=at(dx, dy), device_id_type=MESH)

    sent = []

    def send(src, dst, dx, dy):
        n = len(sent)
        copy = pltpu.make_async_remote_copy(
            src_ref=src,
            dst_ref=dst,
            send_sem=send_sem.at[n],
            recv_sem=recv_sem.at[n],
            device_id=at(dx, dy),
            device_id_type=MESH,
        )
        copy.start()
        sent.append(copy)
        return copy

    loads[0].wait()
    moments, speeds = ([], [])
    for x in range(size_x):
        found = forward([pop[i, x] * np.float32(weights[i]) for i in range(27)])
        rho = found[0]
        inverse = 1.0 / rho
        u = [found[9] * inverse, found[3] * inverse, found[1] * inverse]
        for c in range(3):
            vel[c * rows + x * size_y : c * rows + (x + 1) * size_y, :] = u[c]
        for f, value in enumerate([rho] + u):
            fields[f, x] = value
        moments.append(found)
        speeds.append(u)

    loads[1].wait()
    loads[2].wait()
    for tile in range(slots_all // LANES):
        lanes = slice(tile * LANES, (tile + 1) * LANES)
        cell = stencil[0, 0, :, lanes]
        lane = jnp.bitwise_and(cell, LANES - 1)
        row = jnp.right_shift(cell, 7)
        picked = [jnp.zeros(cell.shape, jnp.float32)] * 3
        for r in range(rows):
            here = row == r
            for c in range(3):
                picked[c] = jnp.where(
                    here, lane_gather(vel[c * rows + r : c * rows + r + 1, :], lane), picked[c]
                )
        factor = weight[0, 0, :, lanes]
        for c in range(3):
            n = tile * 3 + c
            samples[n : n + 1, :] = jnp.sum(picked[c] * factor, axis=0, keepdims=True)
    rx[1, my_y] = samples[...]
    pl.semaphore_wait(barrier, len(greeted))
    sample_copies = [send(samples, rx.at[1 - dx, my_y], dx, dy) for dx, dy in greeted]

    loads[3].wait()
    for side, y in ((0, size_y - 1), (1, 0)):
        for x in range(size_x):
            stage_s[side, x : x + 1, :] = solid[x, y : y + 1, :]
    solid_copies = [
        send(solid.at[size_x - 1], got_sx.at[0], 1, 0),
        send(solid.at[0], got_sx.at[1], -1, 0),
    ]
    for side, dy in ((0, 1), (1, -1)):
        solid_copies.append(send(stage_s.at[side], got_sy.at[side], 0, dy))
        solid_copies.append(send(stage_s.at[side], got_sc.at[0, side], 1, dy))
        solid_copies.append(send(stage_s.at[side], got_sc.at[1, side], -1, dy))

    coefficient = equilibrium_moments()
    for x in range(size_x):
        found, (ux, uy, uz) = (moments[x], speeds[x])
        rho, mx, my, mz = (found[0], found[9], found[3], found[1])
        basis = [rho, mx, my, mz, mx * ux, my * uy, mz * uz, mx * uy, mx * uz, my * uz]
        deviation = []
        for j in range(27):
            if j in (0, 1, 3, 9):
                deviation.append(None)
            else:
                balance = combine(list(zip(coefficient[j], basis)))
                deviation.append(minus(found[j], balance) * relax[j])
        change = backward(deviation)
        for i in range(27):
            half = 0.5 ** int(np.sum(steps[i] != 0)) / weights[i]
            post[i, x] = pop[i, x] - change[i] * np.float32(half)

    for load in loads[4:]:
        load.wait()
    cell = wall[0]
    slot = lax.broadcasted_iota(jnp.int32, (1, slots_all), 1)
    live = slot < count[0, 0]
    which = ref[0]
    offset = lax.rem(my_y * slots, LANES)
    row_hit = jnp.logical_and(
        lax.broadcasted_iota(jnp.int32, (rows, slots_all), 0) == jnp.right_shift(cell, 7), live
    )
    values = [
        jnp.right_shift(which, shift_bits) + 1,
        jnp.bitwise_and(which, slots - 1) + offset,
        jnp.right_shift(normal[0], 1),
    ]
    left = jnp.concatenate(
        [jnp.where(row_hit, value.astype(jnp.float32), 0.0) for value in values], axis=0
    ).astype(jnp.bfloat16)
    right = jnp.where(
        lax.broadcasted_iota(jnp.int32, (LANES, slots_all), 0)
        == jnp.bitwise_and(cell, LANES - 1),
        1.0,
        0.0,
    ).astype(jnp.bfloat16)
    table = lax.dot_general(
        left, right, (((1,), (1,)), ((), ())), preferred_element_type=jnp.float32
    )
    for n in range(3):
        for x in range(size_x):
            first = n * rows + x * size_y
            fields[4 + n, x] = table[first : first + size_y]

    for i in range(27):
        a, b, c = steps[i]
        if b == 0:
            continue
        side = 0 if b > 0 else 1
        edge = size_y - 1 if b > 0 else 0
        for x in range(size_x):
            line = post[i, x, edge : edge + 1, :]
            if 0 <= x + a < size_x:
                n = ((a + 1) * 3 + c + 1) * size_x + x
                stage_y[side, n : n + 1, :] = line
            else:
                stage_c[0 if a > 0 else 1, side, c + 1 : c + 2, :] = line
    for side, y in ((0, size_y - 1), (1, 0)):
        for f in range(7):
            for x in range(size_x):
                n = f * size_x + x
                stage_f[side, n : n + 1, :] = fields[f, x, y : y + 1, :]
    early = [
        send(post.at[18:27, size_x - 1], got_x.at[0], 1, 0),
        send(post.at[0:9, 0], got_x.at[1], -1, 0),
        send(fields.at[:, size_x - 1], got_fx.at[0], 1, 0),
        send(fields.at[:, 0], got_fx.at[1], -1, 0),
    ]
    for side, dy in ((0, 1), (1, -1)):
        for way, dx in ((0, 1), (1, -1)):
            early.append(send(stage_c.at[way, side], got_c.at[way, side], dx, dy))
            early.append(send(stage_f.at[side], got_fc.at[way, side], dx, dy))
        early.append(send(stage_y.at[side], got_y.at[side], 0, dy))
        early.append(send(stage_f.at[side], got_fy.at[side], 0, dy))

    for copy in sample_copies:
        copy.wait_recv()

    def velocity(field, owner, groups):
        source, lane, axis = [value.astype(jnp.int32) for value in field[4:]]
        lane = jnp.bitwise_and(lane, LANES - 1)
        tile = (owner * slots) // LANES
        new = []
        for c in range(3):
            value = jnp.zeros((size_y, LANES), jnp.float32)
            for group, mask in groups:
                for peer in range(devices_y):
                    here = source == peer + 1
                    if mask is not None:
                        here = jnp.logical_and(here, mask)
                    line = rx[group, peer, pl.ds(tile * 3 + c, 1), :]
                    value = jnp.where(here, lane_gather(line, lane), value)
            value = jnp.where(axis == c, 0.0, value * np.float32(wall_ratio))
            new.append(jnp.where(source > 0, value, field[1 + c]))
        return new

    def correction(rho, u, new, wanted):
        linear = [3.0 * rho * (new[c] - u[c]) for c in range(3)]
        pure = [rho * (new[c] * new[c] - u[c] * u[c]) for c in range(3)]
        rest = -1.5 * (pure[0] + pure[1] + pure[2])
        pure = [4.5 * value for value in pure]
        mixed = {
            (c, d): 9.0 * rho * (new[c] * new[d] - u[c] * u[d])
            for c, d in ((0, 1), (0, 2), (1, 2))
        }
        halves, found = ({}, {})
        for i in wanted:
            first = min(i, 26 - i)
            if first not in halves:
                step = steps[first]
                even, odd = (rest, None)
                for c in range(3):
                    if step[c] != 0:
                        even = even + pure[c]
                        odd = plus(odd, linear[c]) if step[c] > 0 else minus(odd, linear[c])
                for c, d in mixed:
                    if step[c] * step[d] > 0:
                        even = even + mixed[c, d]
                    elif step[c] * step[d] < 0:
                        even = even - mixed[c, d]
                halves[first] = (even, odd)
            even, odd = halves[first]
            found[i] = even if odd is None else even + odd if i == first else even - odd
        return found

    for x in range(size_x):
        field = [fields[f, x] for f in range(7)]
        found = correction(field[0], field[1:4], velocity(field, my_y, [(1, None)]), range(27))
        for i in range(27):
            a, b, c = steps[i]
            value = post[i, x] + found[i]
            settled[i, x] = value
            shifted[i, x] = roll(roll(value, b, 0), c, 1)

    for copy in solid_copies:
        copy.wait_recv()
    line_of = lax.broadcasted_iota(jnp.int32, (size_y, LANES), 0)

    def mend(value, line, b):
        edge = 0 if b > 0 else size_y - 1
        return jnp.where(line_of == edge, jnp.broadcast_to(line, value.shape), value)

    for x in range(-1, size_x + 1):
        plane = got_sx[0] if x < 0 else got_sx[1] if x == size_x else solid[x]
        for b in (-1, 0, 1):
            value = roll(plane, b, 0)
            if b != 0:
                side = 0 if b > 0 else 1
                if x < 0:
                    line = got_sc[0, side, size_x - 1 : size_x, :]
                elif x == size_x:
                    line = got_sc[1, side, 0:1, :]
                else:
                    line = got_sy[side, x : x + 1, :]
                value = mend(value, line, b)
            for c in (-1, 0, 1):
                masks[(b + 1) * 3 + c + 1, x + 1] = roll(value, c, 1)

    def gather_rows(target, index, straight, corner, f):
        for x in range(size_x):
            n = f * size_x + x
            target[index + (slice(x, x + 1),)] = straight[n : n + 1, :]
        n = f * size_x + size_x - 1
        target[index + (slice(size_x, size_x + 1),)] = corner[0][n : n + 1, :]
        n = f * size_x
        target[index + (slice(size_x + 1, size_x + 2),)] = corner[1][n : n + 1, :]

    for copy in early:
        copy.wait_recv()
    for side in range(2):
        for j in range(9):
            a, c = (j // 3 - 1, j % 3 - 1)
            for x in range(size_x):
                if 0 <= x + a < size_x:
                    n = j * size_x + x
                    lines[side, j, x : x + 1, :] = got_y[side, n : n + 1, :]
            if a != 0:
                way = 0 if a > 0 else 1
                lines[side, j, size_x + way : size_x + way + 1, :] = got_c[
                    way, side, c + 1 : c + 2, :
                ]
        for f in range(7):
            gather_rows(
                line_fields, (side, f), got_fy.at[side], [got_fc.at[way, side] for way in (0, 1)], f
            )

    border = {}
    for side, b in ((0, 1), (1, -1)):
        wanted = [i for i in range(27) if steps[i][1] == b]
        field = [line_fields[side, f] for f in range(7)]
        owner = lax.rem(my_y + (devices_y - b), devices_y)
        groups = [(1, line_of < size_x), (0, line_of == size_x), (2, line_of == size_x + 1)]
        found = correction(field[0], field[1:4], velocity(field, owner, groups), wanted)
        for i in wanted:
            a, _, c = steps[i]
            border[i] = roll(lines[side, (a + 1) * 3 + c + 1] + found[i], c, 1)
    planes = {}
    for way, a in ((0, 1), (1, -1)):
        wanted = [i for i in range(27) if steps[i][0] == a]
        field = [got_fx[way, f] for f in range(7)]
        found = correction(
            field[0], field[1:4], velocity(field, my_y, [(0 if a > 0 else 2, None)]), wanted
        )
        for i in wanted:
            _, b, c = steps[i]
            planes[i] = roll(roll(got_x[way, i % 9] + found[i], b, 0), c, 1)
    for i in range(27):
        a, b, c = steps[i]
        for x in range(size_x):
            origin = x - a
            inside = 0 <= origin < size_x
            value = shifted[i, origin] if inside else planes[i]
            if b != 0:
                n = origin if inside else size_x + (0 if a > 0 else 1)
                value = mend(value, border[i][n : n + 1, :], b)
            blocked = masks[(b + 1) * 3 + c + 1, origin + 1] != 0
            out[i, x] = jnp.where(blocked, settled[26 - i, x], value)
    for copy in sent:
        copy.wait_send()


def write_out(source, out, sem):
    copy = pltpu.make_async_copy(source, out, sem)
    copy.start()
    copy.wait()


def local(populations, relax, solid, wall_cell, wall_normal, wall_count, sample_ref, cells, factors):
    devices_x, devices_y = (lax.axis_size("gx"), lax.axis_size("gy"))
    size_x, size_y, size_z = populations.shape[1:]
    slots_all = wall_cell.shape[2]
    slots = slots_all // devices_y
    assert size_z == LANES and LANES % slots == 0 and slots & (slots - 1) == 0
    assert slots_all % LANES == 0 and devices_x > 2 and devices_y > 2
    f32, i32 = (jnp.float32, jnp.int32)
    lines = -(-9 * size_x // 8) * 8
    assert size_x + 2 <= size_y == 8
    few = -(-7 * size_x // 8) * 8
    held = -(-3 * slots_all // LANES // 8) * 8
    sends = 3 * devices_y - 1 + 8 + 16
    vmem = pltpu.VMEM
    tile = (size_y, LANES)
    anywhere = pl.BlockSpec(memory_space=pl.ANY)
    smem = pl.BlockSpec(memory_space=pltpu.SMEM)
    result = pl.pallas_call(
        functools.partial(kernel, devices_x, devices_y),
        out_shape=pltpu.VMEM(populations.shape, f32),
        in_specs=[
            anywhere,
            smem,
            anywhere,
            anywhere,
            anywhere,
            smem,
            anywhere,
            anywhere,
            anywhere,
        ],
        out_specs=pl.BlockSpec(memory_space=pltpu.VMEM),
        scratch_shapes=[
            vmem(populations.shape, f32),
            vmem(solid.shape, i32),
            vmem(wall_cell.shape, i32),
            vmem(wall_normal.shape, i32),
            vmem(sample_ref.shape, i32),
            vmem(cells.shape, i32),
            vmem(factors.shape, f32),
            vmem((3 * size_x * size_y, LANES), f32),
            vmem((held, LANES), f32),
            vmem((3, devices_y, held, LANES), f32),
            vmem(populations.shape, f32),
            vmem(populations.shape, f32),
            vmem((7, size_x) + tile, f32),
            vmem(populations.shape, f32),
            vmem((2, lines, LANES), f32),
            vmem((2, 2, 8, LANES), f32),
            vmem((2, 8, LANES), i32),
            vmem((2, few, LANES), f32),
            vmem((2, 9) + tile, f32),
            vmem((2, lines, LANES), f32),
            vmem((2, 2, 8, LANES), f32),
            vmem((2,) + tile, i32),
            vmem((2, 8, LANES), i32),
            vmem((2, 2, 8, LANES), i32),
            vmem((2, 7) + tile, f32),
            vmem((2, few, LANES), f32),
            vmem((2, 2, few, LANES), f32),
            vmem((2, 9, 8, LANES), f32),
            vmem((2, 7, 8, LANES), f32),
            vmem((9, size_x + 2) + tile, i32),
            pltpu.SemaphoreType.DMA((7,)),
            pltpu.SemaphoreType.DMA((sends,)),
            pltpu.SemaphoreType.DMA((sends,)),
        ],
        compiler_params=pltpu.CompilerParams(collective_id=0, has_side_effects=True),
        name="lattice_step",
    )(populations, relax, solid, wall_cell, wall_normal, wall_count, sample_ref, cells, factors)
    result = pltpu.with_memory_space_constraint(result, pltpu.VMEM)
    return pl.pallas_call(
        write_out,
        out_shape=jax.ShapeDtypeStruct(populations.shape, f32),
        in_specs=[pl.BlockSpec(memory_space=pltpu.VMEM)],
        out_specs=anywhere,
        scratch_shapes=[pltpu.SemaphoreType.DMA],
        name="write_out",
    )(result)


def solution(mesh):
    return jax.shard_map(
        local,
        mesh=mesh,
        in_specs=(
            P(None, "gx", "gy", None),
            P(),
            P("gx", "gy", None),
            P("gx", "gy", None),
            P("gx", "gy", None),
            P("gx", "gy"),
            P("gx", "gy", None),
            P("gx", "gy", None, None),
            P("gx", "gy", None, None),
        ),
        out_specs=P(None, "gx", "gy", None),
        check_vma=False,
    )
```

```python
import functools

import jax
import jax.numpy as jnp
import numpy as np
from jax import lax
from jax.experimental import pallas as pl
from jax.experimental.pallas import tpu as pltpu
from jax.sharding import PartitionSpec as P

steps = np.array([(a - 1, b - 1, c - 1) for a in range(3) for b in range(3) for c in range(3)])
wall_ratio = (1.0 / 9.0) ** (1.0 / 7.0)
weights = np.prod(np.where(steps == 0, 2.0 / 3.0, 1.0 / 6.0), axis=1)
vander = np.array([[1.0, 1.0, 1.0], [-1.0, 0.0, 1.0], [1.0, 0.0, 1.0]])
moment = np.kron(np.kron(vander, vander), vander)
LANES = 128
MESH = pl.DeviceIdType.MESH


def equilibrium_moments():
    x, y, z = steps.T.astype(float)
    basis = np.stack(
        [
            np.ones(27),
            3 * x,
            3 * y,
            3 * z,
            4.5 * x * x - 1.5,
            4.5 * y * y - 1.5,
            4.5 * z * z - 1.5,
            9 * x * y,
            9 * x * z,
            9 * y * z,
        ],
        axis=1,
    )
    return moment @ (weights[:, None] * basis)


def forward(vals):
    for stride in (9, 3, 1):
        out = list(vals)
        for i in range(27):
            if i // stride % 3 == 0:
                lo, mid, hi = (vals[i], vals[i + stride], vals[i + 2 * stride])
                both = lo + hi
                out[i], out[i + stride], out[i + 2 * stride] = (both + mid, hi - lo, both)
        vals = out
    return vals


def plus(a, b):
    return b if a is None else a if b is None else a + b


def minus(a, b):
    return a if b is None else -b if a is None else a - b


def backward(vals):
    for stride in (9, 3, 1):
        out = list(vals)
        for i in range(27):
            if i // stride % 3 == 0:
                s0, s1, s2 = (vals[i], vals[i + stride], vals[i + 2 * stride])
                out[i], out[i + stride], out[i + 2 * stride] = (
                    minus(s2, s1),
                    minus(s0, s2),
                    plus(s2, s1),
                )
        vals = out
    return vals


def combine(terms):
    total = None
    for factor, value in terms:
        if abs(factor) < 1e-12:
            continue
        if abs(factor - 1.0) < 1e-12:
            total = plus(total, value)
        elif abs(factor + 1.0) < 1e-12:
            total = minus(total, value)
        else:
            total = plus(total, value * np.float32(factor))
    return total


def roll(value, shift, axis):
    return value if shift == 0 else pltpu.roll(value, shift % value.shape[axis], axis)


def lane_gather(row, index):
    return jnp.take_along_axis(
        jnp.broadcast_to(row, index.shape), index, axis=1, mode="promise_in_bounds"
    )


def kernel(
    devices_x,
    devices_y,
    pop_hbm,
    relax,
    solid_hbm,
    wall_hbm,
    normal_hbm,
    count,
    ref_hbm,
    stencil_hbm,
    weight_hbm,
    out,
    pop,
    solid,
    wall,
    normal,
    ref,
    stencil,
    weight,
    vel,
    samples,
    rx,
    post,
    settled,
    fields,
    shifted,
    stage_y,
    stage_c,
    stage_s,
    stage_f,
    stage_d,
    got_x,
    got_y,
    got_c,
    got_sx,
    got_sy,
    got_fx,
    got_fy,
    got_fc,
    lines,
    line_fields,
    masks,
    load_sem,
    send_sem,
    recv_sem,
):
    size_x, size_y = pop.shape[1:3]
    rows = size_x * size_y
    slots_all = wall.shape[2]
    slots = slots_all // devices_y
    shift_bits = slots.bit_length() - 1
    my_x = lax.axis_index("gx")
    my_y = lax.axis_index("gy")

    def at(dx, dy):
        return {
            "gx": lax.rem(my_x + (dx + devices_x), devices_x),
            "gy": lax.rem(my_y + (dy + devices_y), devices_y),
        }

    loads = [
        pltpu.make_async_copy(src, dst, load_sem.at[n])
        for n, (src, dst) in enumerate(
            [
                (pop_hbm, pop),
                (stencil_hbm, stencil),
                (weight_hbm, weight),
                (solid_hbm, solid),
                (wall_hbm, wall),
                (normal_hbm, normal),
                (ref_hbm, ref),
            ]
        )
    ]
    for load in loads:
        load.start()
    greeted = [(dx, dy) for dx in (-1, 0, 1) for dy in range(devices_y) if (dx, dy) != (0, 0)]
    barrier = pltpu.get_barrier_semaphore()
    for dx, dy in greeted:
        pl.semaphore_signal(barrier, inc=1, device_id=at(dx, dy), device_id_type=MESH)

    sent = []

    def send(src, dst, dx, dy):
        n = len(sent)
        copy = pltpu.make_async_remote_copy(
            src_ref=src,
            dst_ref=dst,
            send_sem=send_sem.at[n],
            recv_sem=recv_sem.at[n],
            device_id=at(dx, dy),
            device_id_type=MESH,
        )
        copy.start()
        sent.append(copy)
        return copy

    loads[0].wait()
    moments, speeds = ([], [])
    for x in range(size_x):
        found = forward([pop[i, x] * np.float32(weights[i]) for i in range(27)])
        rho = found[0]
        inverse = 1.0 / rho
        u = [found[9] * inverse, found[3] * inverse, found[1] * inverse]
        for c in range(3):
            vel[c * rows + x * size_y : c * rows + (x + 1) * size_y, :] = u[c]
        for f, value in enumerate([rho] + u):
            fields[f, x] = value
        moments.append(found)
        speeds.append(u)

    loads[1].wait()
    loads[2].wait()
    for tile in range(slots_all // LANES):
        lanes = slice(tile * LANES, (tile + 1) * LANES)
        cell = stencil[0, 0, :, lanes]
        lane = jnp.bitwise_and(cell, LANES - 1)
        row = jnp.right_shift(cell, 7)
        picked = [jnp.zeros(cell.shape, jnp.float32)] * 3
        for r in range(rows):
            here = row == r
            for c in range(3):
                picked[c] = jnp.where(
                    here, lane_gather(vel[c * rows + r : c * rows + r + 1, :], lane), picked[c]
                )
        factor = weight[0, 0, :, lanes]
        for c in range(3):
            n = tile * 3 + c
            samples[n : n + 1, :] = jnp.sum(picked[c] * factor, axis=0, keepdims=True)
    rx[1, my_y] = samples[...]

    loads[3].wait()
    for side, y in ((0, size_y - 1), (1, 0)):
        for x in range(size_x):
            stage_s[side, x : x + 1, :] = solid[x, y : y + 1, :]

    coefficient = equilibrium_moments()
    for x in range(size_x):
        found, (ux, uy, uz) = (moments[x], speeds[x])
        rho, mx, my, mz = (found[0], found[9], found[3], found[1])
        basis = [rho, mx, my, mz, mx * ux, my * uy, mz * uz, mx * uy, mx * uz, my * uz]
        deviation = []
        for j in range(27):
            if j in (0, 1, 3, 9):
                deviation.append(None)
            else:
                balance = combine(list(zip(coefficient[j], basis)))
                deviation.append(minus(found[j], balance) * relax[j])
        change = backward(deviation)
        for i in range(27):
            half = 0.5 ** int(np.sum(steps[i] != 0)) / weights[i]
            post[i, x] = pop[i, x] - change[i] * np.float32(half)

    for load in loads[4:]:
        load.wait()
    cell = wall[0]
    slot = lax.broadcasted_iota(jnp.int32, (1, slots_all), 1)
    live = slot < count[0, 0]
    which = ref[0]
    offset = lax.rem(my_y * slots, LANES)
    row_hit = jnp.logical_and(
        lax.broadcasted_iota(jnp.int32, (rows, slots_all), 0) == jnp.right_shift(cell, 7), live
    )
    values = [
        jnp.right_shift(which, shift_bits) + 1,
        jnp.bitwise_and(which, slots - 1) + offset,
        jnp.right_shift(normal[0], 1),
    ]
    left = jnp.concatenate(
        [jnp.where(row_hit, value.astype(jnp.float32), 0.0) for value in values], axis=0
    ).astype(jnp.bfloat16)
    right = jnp.where(
        lax.broadcasted_iota(jnp.int32, (LANES, slots_all), 0)
        == jnp.bitwise_and(cell, LANES - 1),
        1.0,
        0.0,
    ).astype(jnp.bfloat16)
    table = lax.dot_general(
        left, right, (((1,), (1,)), ((), ())), preferred_element_type=jnp.float32
    )
    for n in range(3):
        for x in range(size_x):
            first = n * rows + x * size_y
            fields[4 + n, x] = table[first : first + size_y]

    for i in range(27):
        a, b, c = steps[i]
        if b == 0:
            continue
        side = 0 if b > 0 else 1
        edge = size_y - 1 if b > 0 else 0
        for x in range(size_x):
            line = post[i, x, edge : edge + 1, :]
            if 0 <= x + a < size_x:
                n = ((a + 1) * 3 + c + 1) * size_x + x
                stage_y[side, n : n + 1, :] = line
            else:
                stage_c[0 if a > 0 else 1, side, c + 1 : c + 2, :] = line
    for side, y in ((0, size_y - 1), (1, 0)):
        for f in range(7):
            for x in range(size_x):
                n = f * size_x + x
                stage_f[side, n : n + 1, :] = fields[f, x, y : y + 1, :]
            for way, x in ((0, size_x - 1), (1, 0)):
                stage_d[way, side, f : f + 1, :] = fields[f, x, y : y + 1, :]
        for way, x in ((0, size_x - 1), (1, 0)):
            stage_d[way, side, 7:8, :] = solid[x, y : y + 1, :].astype(jnp.float32)
    pl.semaphore_wait(barrier, len(greeted))
    sample_copies = [send(samples, rx.at[1 - dx, my_y], dx, dy) for dx, dy in greeted]
    solid_copies = [
        send(solid.at[size_x - 1], got_sx.at[0], 1, 0),
        send(solid.at[0], got_sx.at[1], -1, 0),
    ]
    for side, dy in ((0, 1), (1, -1)):
        solid_copies.append(send(stage_s.at[side], got_sy.at[side], 0, dy))
    early = [
        send(post.at[18:27, size_x - 1], got_x.at[0], 1, 0),
        send(post.at[0:9, 0], got_x.at[1], -1, 0),
        send(fields.at[:, size_x - 1], got_fx.at[0], 1, 0),
        send(fields.at[:, 0], got_fx.at[1], -1, 0),
    ]
    for side, dy in ((0, 1), (1, -1)):
        for way, dx in ((0, 1), (1, -1)):
            early.append(send(stage_c.at[way, side], got_c.at[way, side], dx, dy))
            early.append(send(stage_d.at[way, side], got_fc.at[way, side], dx, dy))
        early.append(send(stage_y.at[side], got_y.at[side], 0, dy))
        early.append(send(stage_f.at[side], got_fy.at[side], 0, dy))

    for copy in sample_copies:
        copy.wait_recv()

    def velocity(field, owner, groups):
        source, lane, axis = [value.astype(jnp.int32) for value in field[4:]]
        lane = jnp.bitwise_and(lane, LANES - 1)
        tile = (owner * slots) // LANES
        new = []
        for c in range(3):
            value = jnp.zeros((size_y, LANES), jnp.float32)
            for group, mask in groups:
                for peer in range(devices_y):
                    here = source == peer + 1
                    if mask is not None:
                        here = jnp.logical_and(here, mask)
                    line = rx[group, peer, pl.ds(tile * 3 + c, 1), :]
                    value = jnp.where(here, lane_gather(line, lane), value)
            value = jnp.where(axis == c, 0.0, value * np.float32(wall_ratio))
            new.append(jnp.where(source > 0, value, field[1 + c]))
        return new

    def correction(rho, u, new, wanted):
        linear = [3.0 * rho * (new[c] - u[c]) for c in range(3)]
        pure = [rho * (new[c] * new[c] - u[c] * u[c]) for c in range(3)]
        rest = -1.5 * (pure[0] + pure[1] + pure[2])
        pure = [4.5 * value for value in pure]
        mixed = {
            (c, d): 9.0 * rho * (new[c] * new[d] - u[c] * u[d])
            for c, d in ((0, 1), (0, 2), (1, 2))
        }
        halves, found = ({}, {})
        for i in wanted:
            first = min(i, 26 - i)
            if first not in halves:
                step = steps[first]
                even, odd = (rest, None)
                for c in range(3):
                    if step[c] != 0:
                        even = even + pure[c]
                        odd = plus(odd, linear[c]) if step[c] > 0 else minus(odd, linear[c])
                for c, d in mixed:
                    if step[c] * step[d] > 0:
                        even = even + mixed[c, d]
                    elif step[c] * step[d] < 0:
                        even = even - mixed[c, d]
                halves[first] = (even, odd)
            even, odd = halves[first]
            found[i] = even if odd is None else even + odd if i == first else even - odd
        return found

    for x in range(size_x):
        field = [fields[f, x] for f in range(7)]
        found = correction(field[0], field[1:4], velocity(field, my_y, [(1, None)]), range(27))
        for i in range(27):
            a, b, c = steps[i]
            value = post[i, x] + found[i]
            settled[i, x] = value
            shifted[i, x] = roll(roll(value, b, 0), c, 1)

    for copy in solid_copies:
        copy.wait_recv()
    line_of = lax.broadcasted_iota(jnp.int32, (size_y, LANES), 0)

    def mend(value, line, b):
        edge = 0 if b > 0 else size_y - 1
        return jnp.where(line_of == edge, jnp.broadcast_to(line, value.shape), value)

    def mark(x):
        plane = got_sx[0] if x < 0 else got_sx[1] if x == size_x else solid[x]
        for b in (-1, 0, 1):
            value = roll(plane, b, 0)
            if b != 0:
                side = 0 if b > 0 else 1
                if x < 0:
                    line = got_fc[0, side, 7:8, :].astype(jnp.int32)
                elif x == size_x:
                    line = got_fc[1, side, 7:8, :].astype(jnp.int32)
                else:
                    line = got_sy[side, x : x + 1, :]
                value = mend(value, line, b)
            for c in (-1, 0, 1):
                masks[(b + 1) * 3 + c + 1, x + 1] = roll(value, c, 1)

    for x in range(size_x):
        mark(x)

    def gather_rows(target, index, straight, corner, f):
        for x in range(size_x):
            n = f * size_x + x
            target[index + (slice(x, x + 1),)] = straight[n : n + 1, :]
        target[index + (slice(size_x, size_x + 1),)] = corner[0][f : f + 1, :]
        target[index + (slice(size_x + 1, size_x + 2),)] = corner[1][f : f + 1, :]

    for copy in early:
        copy.wait_recv()
    mark(-1)
    mark(size_x)
    for side in range(2):
        for j in range(9):
            a, c = (j // 3 - 1, j % 3 - 1)
            for x in range(size_x):
                if 0 <= x + a < size_x:
                    n = j * size_x + x
                    lines[side, j, x : x + 1, :] = got_y[side, n : n + 1, :]
            if a != 0:
                way = 0 if a > 0 else 1
                lines[side, j, size_x + way : size_x + way + 1, :] = got_c[
                    way, side, c + 1 : c + 2, :
                ]
        for f in range(7):
            gather_rows(
                line_fields, (side, f), got_fy.at[side], [got_fc.at[way, side] for way in (0, 1)], f
            )

    border = {}
    for side, b in ((0, 1), (1, -1)):
        wanted = [i for i in range(27) if steps[i][1] == b]
        field = [line_fields[side, f] for f in range(7)]
        owner = lax.rem(my_y + (devices_y - b), devices_y)
        groups = [(1, line_of < size_x), (0, line_of == size_x), (2, line_of == size_x + 1)]
        found = correction(field[0], field[1:4], velocity(field, owner, groups), wanted)
        for i in wanted:
            a, _, c = steps[i]
            border[i] = roll(lines[side, (a + 1) * 3 + c + 1] + found[i], c, 1)
    planes = {}
    for way, a in ((0, 1), (1, -1)):
        wanted = [i for i in range(27) if steps[i][0] == a]
        field = [got_fx[way, f] for f in range(7)]
        found = correction(
            field[0], field[1:4], velocity(field, my_y, [(0 if a > 0 else 2, None)]), wanted
        )
        for i in wanted:
            _, b, c = steps[i]
            planes[i] = roll(roll(got_x[way, i % 9] + found[i], b, 0), c, 1)
    for i in range(27):
        a, b, c = steps[i]
        for x in range(size_x):
            origin = x - a
            inside = 0 <= origin < size_x
            value = shifted[i, origin] if inside else planes[i]
            if b != 0:
                n = origin if inside else size_x + (0 if a > 0 else 1)
                value = mend(value, border[i][n : n + 1, :], b)
            blocked = masks[(b + 1) * 3 + c + 1, origin + 1] != 0
            out[i, x] = jnp.where(blocked, settled[26 - i, x], value)
    for copy in sent:
        copy.wait_send()


def write_out(source, out, sem):
    copy = pltpu.make_async_copy(source, out, sem)
    copy.start()
    copy.wait()


def local(populations, relax, solid, wall_cell, wall_normal, wall_count, sample_ref, cells, factors):
    devices_x, devices_y = (lax.axis_size("gx"), lax.axis_size("gy"))
    size_x, size_y, size_z = populations.shape[1:]
    slots_all = wall_cell.shape[2]
    slots = slots_all // devices_y
    assert size_z == LANES and LANES % slots == 0 and slots & (slots - 1) == 0
    assert slots_all % LANES == 0 and devices_x > 2 and devices_y > 2
    f32, i32 = (jnp.float32, jnp.int32)
    lines = -(-9 * size_x // 8) * 8
    assert size_x + 2 <= size_y == 8
    few = -(-7 * size_x // 8) * 8
    held = -(-3 * slots_all // LANES // 8) * 8
    sends = 3 * devices_y - 1 + 4 + 16
    vmem = pltpu.VMEM
    tile = (size_y, LANES)
    anywhere = pl.BlockSpec(memory_space=pl.ANY)
    smem = pl.BlockSpec(memory_space=pltpu.SMEM)
    result = pl.pallas_call(
        functools.partial(kernel, devices_x, devices_y),
        out_shape=pltpu.VMEM(populations.shape, f32),
        in_specs=[
            anywhere,
            smem,
            anywhere,
            anywhere,
            anywhere,
            smem,
            anywhere,
            anywhere,
            anywhere,
        ],
        out_specs=pl.BlockSpec(memory_space=pltpu.VMEM),
        scratch_shapes=[
            vmem(populations.shape, f32),
            vmem(solid.shape, i32),
            vmem(wall_cell.shape, i32),
            vmem(wall_normal.shape, i32),
            vmem(sample_ref.shape, i32),
            vmem(cells.shape, i32),
            vmem(factors.shape, f32),
            vmem((3 * size_x * size_y, LANES), f32),
            vmem((held, LANES), f32),
            vmem((3, devices_y, held, LANES), f32),
            vmem(populations.shape, f32),
            vmem(populations.shape, f32),
            vmem((7, size_x) + tile, f32),
            vmem(populations.shape, f32),
            vmem((2, lines, LANES), f32),
            vmem((2, 2, 8, LANES), f32),
            vmem((2, 8, LANES), i32),
            vmem((2, few, LANES), f32),
            vmem((2, 2, 8, LANES), f32),
            vmem((2, 9) + tile, f32),
            vmem((2, lines, LANES), f32),
            vmem((2, 2, 8, LANES), f32),
            vmem((2,) + tile, i32),
            vmem((2, 8, LANES), i32),
            vmem((2, 7) + tile, f32),
            vmem((2, few, LANES), f32),
            vmem((2, 2, 8, LANES), f32),
            vmem((2, 9, 8, LANES), f32),
            vmem((2, 7, 8, LANES), f32),
            vmem((9, size_x + 2) + tile, i32),
            pltpu.SemaphoreType.DMA((7,)),
            pltpu.SemaphoreType.DMA((sends,)),
            pltpu.SemaphoreType.DMA((sends,)),
        ],
        compiler_params=pltpu.CompilerParams(collective_id=0, has_side_effects=True),
        name="lattice_step",
    )(populations, relax, solid, wall_cell, wall_normal, wall_count, sample_ref, cells, factors)
    result = pltpu.with_memory_space_constraint(result, pltpu.VMEM)
    return pl.pallas_call(
        write_out,
        out_shape=jax.ShapeDtypeStruct(populations.shape, f32),
        in_specs=[pl.BlockSpec(memory_space=pltpu.VMEM)],
        out_specs=anywhere,
        scratch_shapes=[pltpu.SemaphoreType.DMA],
        name="write_out",
    )(result)


def solution(mesh):
    return jax.shard_map(
        local,
        mesh=mesh,
        in_specs=(
            P(None, "gx", "gy", None),
            P(),
            P("gx", "gy", None),
            P("gx", "gy", None),
            P("gx", "gy", None),
            P("gx", "gy"),
            P("gx", "gy", None),
            P("gx", "gy", None, None),
            P("gx", "gy", None, None),
        ),
        out_specs=P(None, "gx", "gy", None),
        check_vma=False,
    )
```
